32 devices in a mesh: ctx: 4 (over z), fsdp: 8 (over y, x, core).
Axes of the slice: x: 2, y: 2, z: 4, core: 2. Of those that a mesh axis runs over, the one named last changes fastest.
Arguments:
- tokens: bfloat16 [8, 1024, 1536], P('fsdp', 'ctx'), may hold values from -6 to 6
- segments: int32 [8, 1024], P('fsdp', 'ctx'), may hold values from 0 to 1, as said below
- positions: int32 [8, 1024], P('fsdp', 'ctx'), may hold values from 0 to 639, as said below
- out_grad: bfloat16 [8, 1024, 1536], P('fsdp', 'ctx'), may hold values from -6 to 6
- conv_norm: bfloat16 [1536], P('fsdp'), may hold values from 0.099609375 to 1.8984375
- conv_in: bfloat16 [1536, 4608], P('fsdp'), may hold values from -0.15625 to 0.15625
- conv_kernel: bfloat16 [1536, 3], P('fsdp'), may hold values from -3.5 to 3.5
- conv_out: bfloat16 [1536, 1536], P('fsdp'), may hold values from -0.15625 to 0.15625
- ffn_norm_1: bfloat16 [1536], P('fsdp'), may hold values from 0.099609375 to 1.8984375
- gate_up_1: bfloat16 [1536, 13824], P('fsdp'), may hold values from -0.15625 to 0.15625
- down_1: bfloat16 [6912, 1536], P('fsdp'), may hold values from -0.078125 to 0.078125
- attn_norm: bfloat16 [1536], P('fsdp'), may hold values from 0.099609375 to 1.8984375
- qkv_weight: bfloat16 [1536, 2560], P('fsdp'), may hold values from -0.15625 to 0.15625
- q_gain: bfloat16 [64], P('fsdp'), may hold values from 0.099609375 to 1.8984375
- k_gain: bfloat16 [64], P('fsdp'), may hold values from 0.099609375 to 1.8984375
- attn_out: bfloat16 [1536, 1536], P('fsdp'), may hold values from -0.75 to 0.75
- ffn_norm_2: bfloat16 [1536], P('fsdp'), may hold values from 0.099609375 to 1.8984375
- gate_up_2: bfloat16 [1536, 13824], P('fsdp'), may hold values from -0.15625 to 0.15625
- down_2: bfloat16 [6912, 1536], P('fsdp'), may hold values from -0.078125 to 0.078125
Outputs:
- result: bfloat16 [8, 1024, 1536], P('fsdp', 'ctx')
- tokens_grad: float32 [8, 1024, 1536], P('fsdp', 'ctx')
- grad_conv_norm: float32 [1536], P('fsdp')
- grad_conv_in: float32 [1536, 4608], P('fsdp')
- grad_conv_kernel: float32 [1536, 3], P('fsdp')
- grad_conv_out: float32 [1536, 1536], P('fsdp')
- grad_ffn_norm_1: float32 [1536], P('fsdp')
- grad_gate_up_1: float32 [1536, 13824], P('fsdp')
- grad_down_1: float32 [6912, 1536], P('fsdp')
- grad_attn_norm: float32 [1536], P('fsdp')
- grad_qkv_weight: float32 [1536, 2560], P('fsdp')
- grad_q_gain: float32 [64], P('fsdp')
- grad_k_gain: float32 [64], P('fsdp')
- grad_attn_out: float32 [1536, 1536], P('fsdp')
- grad_ffn_norm_2: float32 [1536], P('fsdp')
- grad_gate_up_2: float32 [1536, 13824], P('fsdp')
- grad_down_2: float32 [6912, 1536], P('fsdp')
The draws below stay inside these ranges and needn't reach their ends.
Inputs may be any that keep to these rules, and one draw needn't show every extreme that they name: `segments`: along the sequence order of each sequence the document id never falls, and each of the 2 ids holds at least one row. `positions`: in sequence order a document's first row has position 0 and each following row of the same document one more.
All inputs are finite; a program needn't handle non-finite values.
Results may differ from the reference program's by a relative error of at most 0.03.
Values may be sent and summed in bfloat16 or wider, within the bound.
A program may use at most 640 MiB of HBM per device.

```python
import functools
import jax
import jax.numpy as jnp
import numpy as np
from jax import lax

D = 1536
FF = 6912
HEADS = 24
KV_HEADS = 8
HEAD_DIM = 64
KERNEL = 3
DOCS = 2
BLOCKS = 8
SEQ_LEN = 1024
HALF = 128
SEQS = 8
N_CTX = 4


def stored_from_sequence(array):
    blocks = 2 * N_CTX
    order_table = np.array([2 * seq_block if seq_block < N_CTX else 2 * (blocks - 1 - seq_block) + 1 for seq_block in range(blocks)], dtype=np.int32)
    inverse = np.argsort(order_table).astype(np.int32)
    shaped = array.reshape(SEQS, blocks, SEQ_LEN // blocks)
    return jnp.take(shaped, jnp.asarray(inverse), axis=1).reshape(SEQS, SEQ_LEN).astype(jnp.int32)


def document_layout(key):
    inner_key = jax.random.fold_in(key, 11)
    starts = jnp.arange(1, DOCS, dtype=jnp.int32) * (SEQ_LEN // DOCS)
    spread = SEQ_LEN // (4 * DOCS)
    sides = jax.random.randint(inner_key, (SEQS, DOCS - 1), 0, 2, dtype=jnp.int32)
    offsets = spread * (2 * sides - 1)
    bounds = starts[None, :] + offsets
    place = jnp.arange(SEQ_LEN, dtype=jnp.int32)
    after = place[None, :, None] >= bounds[:, None, :]
    doc_ids = jnp.sum(after.astype(jnp.int32), axis=-1)
    doc_start = jnp.max(jnp.where(after, bounds[:, None, :], 0), axis=-1)
    return (doc_ids, place[None, :] - doc_start)


def draw_segments(key, part):
    doc_ids, offsets = document_layout(key)
    return stored_from_sequence(doc_ids)


def draw_positions(key, part):
    doc_ids, offsets = document_layout(key)
    return stored_from_sequence(offsets)


def shard_levels(stream_key, dims, split, smallest, top_value):
    def one(dim, parts):
        steps = jax.random.uniform(jax.random.fold_in(jax.random.fold_in(stream_key, 6), dim), (parts,), jnp.float32, smallest / len(split), top_value / len(split))
        return jnp.repeat(jnp.exp(steps), dims[dim] // parts).reshape((-1,) + (1,) * (len(dims) - dim - 1))

    loudness = one(*split[0])
    for cut in split[1:]:
        loudness = loudness * one(*cut)
    return loudness


def gaussian(key, shape, width, limit, pieces=(), kind=jnp.bfloat16):
    values = jax.random.normal(key, shape, jnp.float32) * width
    if len(pieces) > 0:
        values = shard_levels(key, shape, pieces, -0.22, 0.18) * values
    return jnp.clip(values, min=-limit, max=limit).astype(kind)


def setup_inputs(seed: int = 0) -> dict:
    seeds = jax.random.split(jax.random.key(seed), 20)
    return {
        "tokens": gaussian(seeds[0], (SEQS, SEQ_LEN, D), 1.0, 6.0, ((0, 8), (1, 4))),
        "segments": draw_segments(jax.random.fold_in(seeds[19], 71), 0),
        "positions": draw_positions(jax.random.fold_in(seeds[19], 71), 0),
        "out_grad": gaussian(seeds[3], (SEQS, SEQ_LEN, D), 1.0, 6.0, ((0, 8), (1, 4))),
        "conv_norm": jnp.clip(1.0 + 0.18 * jax.random.normal(seeds[4], (D,), jnp.float32), 0.099609375, 1.8984375).astype(jnp.bfloat16),
        "conv_in": gaussian(seeds[5], (D, 3 * D), D ** -0.5, 0.15625, ((0, 8),)),
        "conv_kernel": gaussian(seeds[6], (D, KERNEL), KERNEL ** -0.5, 3.5, ((0, 8),)),
        "conv_out": gaussian(seeds[7], (D, D), D ** -0.5, 0.15625, ((0, 8),)),
        "ffn_norm_1": jnp.clip(1.0 + 0.18 * jax.random.normal(seeds[8], (D,), jnp.float32), 0.099609375, 1.8984375).astype(jnp.bfloat16),
        "gate_up_1": gaussian(seeds[9], (D, 2 * FF), D ** -0.5, 0.15625, ((0, 8),)),
        "down_1": gaussian(seeds[10], (FF, D), FF ** -0.5, 0.078125, ((0, 8),)),
        "attn_norm": jnp.clip(1.0 + 0.18 * jax.random.normal(seeds[11], (D,), jnp.float32), 0.099609375, 1.8984375).astype(jnp.bfloat16),
        "qkv_weight": gaussian(seeds[12], (D, (HEADS + 2 * KV_HEADS) * HEAD_DIM), D ** -0.5, 0.15625, ((0, 8),)),
        "q_gain": jnp.clip(1.0 + 0.18 * jax.random.normal(seeds[13], (HEAD_DIM,), jnp.float32), 0.099609375, 1.8984375).astype(jnp.bfloat16),
        "k_gain": jnp.clip(1.0 + 0.18 * jax.random.normal(seeds[14], (HEAD_DIM,), jnp.float32), 0.099609375, 1.8984375).astype(jnp.bfloat16),
        "attn_out": gaussian(seeds[15], (HEADS * HEAD_DIM, D), (HEADS * HEAD_DIM // 24) ** -0.5, 0.75, ((0, 8),)),
        "ffn_norm_2": jnp.clip(1.0 + 0.18 * jax.random.normal(seeds[16], (D,), jnp.float32), 0.099609375, 1.8984375).astype(jnp.bfloat16),
        "gate_up_2": gaussian(seeds[17], (D, 2 * FF), D ** -0.5, 0.15625, ((0, 8),)),
        "down_2": gaussian(seeds[18], (FF, D), FF ** -0.5, 0.078125, ((0, 8),)),
    }


EPSILON = 1e-05
ROPE_BASE = 1000000.0
MASKED = -1e+30

@jax.custom_vjp
def low(v):
    return lax.optimization_barrier(v.astype(jnp.bfloat16)).astype(jnp.float32)

@jax.custom_vjp
def low_back(v):
    return v

def low_keep(v):
    return (low(v), None)

def low_pass(kept, grad):
    return (grad,)

def back_keep(v):
    return (v, None)

def back_low(kept, grad):
    return (low(grad),)
low.defvjp(low_keep, low_pass)
low_back.defvjp(back_keep, back_low)

def block_order():
    blocks = 2 * N_CTX
    return np.array([2 * seq_block if seq_block < N_CTX else 2 * (blocks - 1 - seq_block) + 1 for seq_block in range(blocks)], dtype=np.int32)

def to_sequence(array):
    shaped = array.reshape((SEQS, BLOCKS, HALF) + array.shape[2:])
    return jnp.take(shaped, jnp.asarray(block_order()), axis=1).reshape(array.shape)

def to_stored(array):
    shaped = array.reshape((SEQS, BLOCKS, HALF) + array.shape[2:])
    inverse = np.argsort(block_order()).astype(np.int32)
    return jnp.take(shaped, jnp.asarray(inverse), axis=1).reshape(array.shape)

def rms_norm(values, gain_vec):
    return values * lax.rsqrt(lax.optimization_barrier(jnp.mean(values * values, axis=-1, keepdims=True)) + EPSILON) * gain_vec

def matmul_high(left_arr, right_arr):
    return jnp.dot(left_arr, right_arr, precision=lax.Precision.HIGHEST, preferred_element_type=jnp.float32)

def rotary_tables(places):
    exponent = jnp.arange(HEAD_DIM // 2, dtype=jnp.float32) * 2.0 / HEAD_DIM
    inverse = jnp.power(ROPE_BASE, -exponent)
    angles = places.astype(jnp.float32)[:, None] * inverse[None, :]
    angles = jnp.concatenate([angles, angles], axis=-1)
    return (jnp.cos(angles)[:, None, :], jnp.sin(angles)[:, None, :])

def rotary(field_in, cosine, sine_tab):
    half_dim = field_in.shape[-1] // 2
    turned = jnp.concatenate([-field_in[..., half_dim:], field_in[..., :half_dim]], axis=-1)
    return field_in * cosine + turned * sine_tab

def head_parts(mixed_in, q_gain_vec, k_gain_vec, cosine, sine_tab):
    row_count = mixed_in.shape[0]
    q_width = HEADS * HEAD_DIM
    kv_width = KV_HEADS * HEAD_DIM
    queries = mixed_in[:, :q_width].reshape(row_count, HEADS, HEAD_DIM)
    keys_part = mixed_in[:, q_width:q_width + kv_width].reshape(row_count, KV_HEADS, HEAD_DIM)
    values = mixed_in[:, q_width + kv_width:]
    queries = rotary(rms_norm(queries, q_gain_vec), cosine, sine_tab)
    keys_part = rotary(rms_norm(keys_part, k_gain_vec), cosine, sine_tab)
    return (queries.reshape(row_count, q_width), keys_part.reshape(row_count, kv_width), values)

def attend_one(packed):
    queries, keys_part, values, doc_ids, places = packed
    allowed = (places[:, None] >= places[None, :]) & (doc_ids[:, None] == doc_ids[None, :])
    raw_scores = jnp.einsum('tkgd,skd->kgts', queries, keys_part, precision=lax.Precision.HIGHEST)
    scores = low_back(raw_scores * HEAD_DIM ** (-0.5))
    log_total = jax.nn.logsumexp(jnp.where(allowed, scores, MASKED), axis=-1, keepdims=True)
    weights = jnp.where(allowed, jnp.exp(scores - log_total), 0.0)
    mixed_out = jnp.einsum('kgts,skd->tkgd', low(weights), values, precision=lax.Precision.HIGHEST)
    return low_back(mixed_out)

def conv_branch(values, gain_vec, w_in, kernel, w_out):
    normed = low(rms_norm(values, gain_vec))
    mixed_out = low_back(matmul_high(normed, w_in))
    gate_b = mixed_out[:, :D]
    gate_c = mixed_out[:, D:2 * D]
    inner_val = mixed_out[:, 2 * D:]
    product = low(gate_b * inner_val).reshape(SEQS, SEQ_LEN, D)
    padded = jnp.pad(product, ((0, 0), (KERNEL - 1, 0), (0, 0)))
    convolved = jnp.zeros_like(product)
    for offset in range(KERNEL):
        convolved = convolved + padded[:, offset:offset + SEQ_LEN] * kernel[:, offset]
    gated_low = low(gate_c * convolved.reshape(-1, D))
    return low_back(matmul_high(gated_low, w_out))

def ffn_branch(values, gain_vec, w_gate_up, w_down):
    normed = low(rms_norm(values, gain_vec))
    mixed_out = low_back(matmul_high(normed, w_gate_up))
    hidden = low(jax.nn.silu(mixed_out[:, :FF]) * mixed_out[:, FF:])
    return low_back(matmul_high(hidden, w_down))

def attention_branch(values, gain_vec, w_qkv, q_gain_vec, k_gain_vec, w_out, doc_ids, places):
    normed = low(rms_norm(values, gain_vec))
    mixed_out = low_back(matmul_high(normed, w_qkv))
    cosine, sine_tab = rotary_tables(places.reshape(-1))
    queries, keys_part, value_part = head_parts(mixed_out, q_gain_vec, k_gain_vec, cosine, sine_tab)
    groups = HEADS // KV_HEADS
    queries = low(queries).reshape(SEQS, SEQ_LEN, KV_HEADS, groups, HEAD_DIM)
    keys_part = low(keys_part).reshape(SEQS, SEQ_LEN, KV_HEADS, HEAD_DIM)
    value_part = low(value_part).reshape(SEQS, SEQ_LEN, KV_HEADS, HEAD_DIM)
    attended = lax.map(jax.checkpoint(attend_one), (queries, keys_part, value_part, doc_ids, places))
    attended = low(attended.reshape(SEQS * SEQ_LEN, HEADS * HEAD_DIM))
    return low_back(matmul_high(attended, w_out))

def forward(doc_ids, places, start, conv_norm, conv_in, conv_kernel, conv_out, ffn_norm_1, gate_up_1, down_1, attn_norm, qkv_weight, q_gain, k_gain, attn_out, ffn_norm_2, gate_up_2, down_2):
    hidden = start + conv_branch(start, conv_norm, conv_in, conv_kernel, conv_out)
    hidden = hidden + ffn_branch(hidden, ffn_norm_1, gate_up_1, down_1)
    hidden = hidden + attention_branch(hidden, attn_norm, qkv_weight, q_gain, k_gain, attn_out, doc_ids, places)
    return hidden + ffn_branch(hidden, ffn_norm_2, gate_up_2, down_2)

def reference(tokens, segments, positions, out_grad, conv_norm, conv_in, conv_kernel, conv_out, ffn_norm_1, gate_up_1, down_1, attn_norm, qkv_weight, q_gain, k_gain, attn_out, ffn_norm_2, gate_up_2, down_2):
    params = tuple((weight_arr.astype(jnp.float32) for weight_arr in (conv_norm, conv_in, conv_kernel, conv_out, ffn_norm_1, gate_up_1, down_1, attn_norm, qkv_weight, q_gain, k_gain, attn_out, ffn_norm_2, gate_up_2, down_2)))
    doc_ids = to_sequence(segments)
    places = to_sequence(positions)
    start = to_sequence(tokens.astype(jnp.float32)).reshape(-1, D)
    output, backward = jax.vjp(functools.partial(forward, doc_ids, places), start, *params)
    cotangent = to_sequence(out_grad.astype(jnp.float32)).reshape(-1, D)
    grads = backward(cotangent)
    result = to_stored(output.reshape(SEQS, SEQ_LEN, D)).astype(jnp.bfloat16)
    tokens_grad = to_stored(grads[0].reshape(SEQS, SEQ_LEN, D))
    return (result, tokens_grad, grads[1], grads[2], grads[3], grads[4], grads[5], grads[6], grads[7], grads[8], grads[9], grads[10], grads[11], grads[12], grads[13], grads[14], grads[15])
```

```python
import functools

import jax
import jax.numpy as jnp
from jax import lax
from jax.experimental import pallas as pl
from jax.experimental.pallas import tpu as pltpu
from jax.sharding import PartitionSpec as P

HEADS = 24
KV_HEADS = 8
HEAD_DIM = 64
KERNEL = 3


EPSILON = 1e-05
ROPE_BASE = 1000000.0
MASKED = -1e30
SPLIT_BASE = 64
LANES = 128
TILE = 256
SUBLANES = 16
VMEM_LIMIT = 60 * 1024 * 1024
MESH = pl.DeviceIdType.MESH


def silu_parts(gate):
    sig = 1.0 / (1.0 + jnp.exp(-gate))
    return sig, gate * sig


def dot_tb(a, b):
    return lax.dot_general(a, b, (((1,), (1,)), ((), ())), preferred_element_type=jnp.float32)


def dot_ta(a, b):
    return lax.dot_general(a, b, (((0,), (0,)), ((), ())), preferred_element_type=jnp.float32)


def accumulate(step, acc_ref, term):
    @pl.when(step == 0)
    def _():
        acc_ref[...] = term

    @pl.when(step > 0)
    def _():
        acc_ref[...] += term


def load_rows(all_ref, refs):
    at = 0
    for ref in refs:
        all_ref[at : at + ref.shape[0]] = ref[...]
        at += ref.shape[0]


def store_rows(refs, all_ref):
    at = 0
    for ref in refs:
        ref[...] = all_ref[at : at + ref.shape[0]].astype(ref.dtype)
        at += ref.shape[0]


def whole_block(value):
    return pl.BlockSpec(value.shape, lambda j: (0, 0), pipeline_mode=pl.Buffered(1))


def column_block(rows):
    return pl.BlockSpec((rows, TILE), lambda j: (0, j))


def low_shape(*shape):
    return jax.ShapeDtypeStruct(shape, jnp.bfloat16)


def cost(flops, moved, special=0):
    return pl.CostEstimate(flops=flops, bytes_accessed=moved, transcendentals=special)


def ffn_fwd_kernel(count, *refs):
    ns = refs[:count]
    wg_ref, wu_ref, wd_ref, gate_ref, up_ref, hid_ref = refs[count : count + 6]
    outs = refs[count + 6 : 2 * count + 6]
    n_all, acc_ref = refs[2 * count + 6 :]
    step = pl.program_id(0)

    @pl.when(step == 0)
    def _():
        load_rows(n_all, ns)

    gate = jnp.dot(n_all[...], wg_ref[...], preferred_element_type=jnp.float32)
    up = jnp.dot(n_all[...], wu_ref[...], preferred_element_type=jnp.float32)
    gate_ref[...] = gate.astype(jnp.bfloat16)
    up_ref[...] = up.astype(jnp.bfloat16)
    hid = (silu_parts(gate)[1] * up).astype(jnp.bfloat16)
    hid_ref[...] = hid
    accumulate(step, acc_ref, jnp.dot(hid, wd_ref[...], preferred_element_type=jnp.float32))

    @pl.when(step == pl.num_programs(0) - 1)
    def _():
        store_rows(outs, acc_ref)


def ffn_fwd(ns, wg, wu, wd):
    width, d = wd.shape
    rows = sum(n.shape[0] for n in ns)
    wide = pl.BlockSpec((d, TILE), lambda j: (0, j))
    col = column_block(rows)
    out = pl.pallas_call(
        functools.partial(ffn_fwd_kernel, len(ns)),
        grid=(width // TILE,),
        in_specs=[whole_block(n) for n in ns]
        + [wide, wide, pl.BlockSpec((TILE, d), lambda j: (j, 0))],
        out_specs=[col, col, col] + [pl.BlockSpec(n.shape, lambda j: (0, 0)) for n in ns],
        out_shape=[low_shape(rows, width)] * 3 + [low_shape(*n.shape) for n in ns],
        scratch_shapes=[pltpu.VMEM((rows, d), jnp.bfloat16), pltpu.VMEM((rows, d), jnp.float32)],
        compiler_params=pltpu.CompilerParams(vmem_limit_bytes=VMEM_LIMIT),
        cost_estimate=cost(
            6 * rows * d * width, 6 * d * width + 6 * rows * width + 4 * rows * d, rows * width
        ),
        name="ffn_fwd",
    )(*ns, wg, wu, wd)
    return out[0], out[1], out[2], list(out[3:])


def ffn_grads_kernel(count, parts, rows_d, *refs):
    gs = refs[:count]
    ns = refs[count : 2 * count]
    at = 2 * count
    gates, ups, hids = (refs[at + i * parts : at + (i + 1) * parts] for i in range(3))
    at += 3 * parts
    wd_ref, dg_ref, du_ref, mine_ref, theirs_ref, gd_ref, g_all, n_all = refs[at:]
    step = pl.program_id(0)

    @pl.when(step == 0)
    def _():
        load_rows(g_all, gs)
        load_rows(n_all, ns)

    def joined(pieces):
        values = [piece[...] for piece in pieces]
        return values[0] if parts == 1 else jnp.concatenate(values, axis=0)

    dhid = dot_tb(g_all[...], wd_ref[...])
    gate = joined(gates).astype(jnp.float32)
    up = joined(ups).astype(jnp.float32)
    sig, act = silu_parts(gate)
    dgate = (dhid * up * (sig + act * (1.0 - sig))).astype(jnp.bfloat16)
    dup = (dhid * act).astype(jnp.bfloat16)
    dg_ref[...] = dgate
    du_ref[...] = dup
    first = lax.axis_index("fsdp") % 2 == 0
    for half, grads in enumerate((dgate, dup)):
        full = dot_ta(n_all[...], grads).astype(jnp.bfloat16)
        for i in range(full.shape[0] // (2 * rows_d)):
            even = full[2 * i * rows_d : (2 * i + 1) * rows_d]
            odd = full[(2 * i + 1) * rows_d : (2 * i + 2) * rows_d]
            mine_ref[half, i * rows_d : (i + 1) * rows_d] = jnp.where(first, even, odd)
            theirs_ref[half, i * rows_d : (i + 1) * rows_d] = jnp.where(first, odd, even)
    gd_ref[...] = dot_ta(joined(hids), g_all[...]).astype(jnp.bfloat16)


def ffn_grads(gs, ns, gates, ups, hids, wd, rows_d):
    width, d = wd.shape
    rows = sum(n.shape[0] for n in ns)
    cols = [column_block(v.shape[0]) for v in gates]
    col = column_block(rows)
    halves = pl.BlockSpec((2, d // 2, TILE), lambda j: (0, 0, j))
    return pl.pallas_call(
        functools.partial(ffn_grads_kernel, len(ns), len(gates), rows_d),
        grid=(width // TILE,),
        in_specs=[whole_block(v) for v in gs]
        + [whole_block(v) for v in ns]
        + cols * 3
        + [pl.BlockSpec((TILE, d), lambda j: (j, 0))],
        out_specs=[col, col, halves, halves, pl.BlockSpec((TILE, d), lambda j: (j, 0))],
        out_shape=[
            low_shape(rows, width),
            low_shape(rows, width),
            low_shape(2, d // 2, width),
            low_shape(2, d // 2, width),
            low_shape(width, d),
        ],
        scratch_shapes=[pltpu.VMEM((rows, d), jnp.bfloat16)] * 2,
        compiler_params=pltpu.CompilerParams(vmem_limit_bytes=VMEM_LIMIT),
        cost_estimate=cost(
            8 * rows * d * width, 8 * d * width + 10 * rows * width + 4 * rows * d, rows * width
        ),
        name="ffn_grads",
    )(*gs, *ns, *gates, *ups, *hids, wd)


def ffn_down_kernel(count, dg_ref, du_ref, wg_ref, wu_ref, *refs):
    step = pl.program_id(0)
    acc_ref = refs[count]
    accumulate(
        step, acc_ref, dot_tb(dg_ref[...], wg_ref[...]) + dot_tb(du_ref[...], wu_ref[...])
    )

    @pl.when(step == pl.num_programs(0) - 1)
    def _():
        store_rows(refs[:count], acc_ref)


def ffn_input_grad(dg, du, wg, wu, count):
    d, width = wg.shape
    rows = dg.shape[0]
    wide = pl.BlockSpec((d, TILE), lambda j: (0, j))
    col = column_block(rows)
    return list(
        pl.pallas_call(
            functools.partial(ffn_down_kernel, count),
            grid=(width // TILE,),
            in_specs=[col, col, wide, wide],
            out_specs=[pl.BlockSpec((rows // count, d), lambda j: (0, 0))] * count,
            out_shape=[low_shape(rows // count, d)] * count,
            scratch_shapes=[pltpu.VMEM((rows, d), jnp.float32)],
            compiler_params=pltpu.CompilerParams(vmem_limit_bytes=VMEM_LIMIT),
            cost_estimate=cost(
                4 * rows * d * width, 4 * d * width + 4 * rows * width + 2 * rows * d
            ),
            name="ffn_input_grad",
        )(dg, du, wg, wu)
    )


def chip_count():
    return lax.axis_size("fsdp") // 2


def chip_index():
    return lax.axis_index("fsdp") // 2


def core_index():
    return lax.axis_index("fsdp") % 2


def flipped(index, step):
    out = index
    bit = 1
    while bit <= step:
        if step & bit:
            out = out + (1 - 2 * ((index // bit) % 2)) * bit
        bit *= 2
    return out


def ring_swap(value, axis, step):
    size = lax.axis_size(axis)
    return lax.ppermute(value, axis, [(i, i ^ step) for i in range(size)])


def chip_swap(value, step):
    return ring_swap(value, "fsdp", 2 * step)


def core_swap(value):
    return ring_swap(value, "fsdp", 1)


def gather_small(value):
    step = 1
    out = value[None]
    while step < lax.axis_size("fsdp"):
        beside = ring_swap(out, "fsdp", step)
        low = (lax.axis_index("fsdp") // step) % 2 == 0
        out = jnp.concatenate([jnp.where(low, out, beside), jnp.where(low, beside, out)], axis=0)
        step *= 2
    return out


def sum_small(value):
    for axis in ("fsdp", "ctx"):
        step = 1
        while step < lax.axis_size(axis):
            value = value + ring_swap(value, axis, step)
            step *= 2
    return value


def gather_chunks(value):
    return [value] + [chip_swap(value, step) for step in range(1, chip_count())]


def scatter_sum(parts):
    total = parts[0].astype(jnp.float32)
    for step in range(1, len(parts)):
        total = total + chip_swap(parts[step], step).astype(jnp.float32)
    return total


def slice_plan(block, chips):
    span = 2 * block
    total = span * chips
    spans = [(q * span // LANES * LANES, (q + 1) * span) for q in range(chips)]
    width = max(-(-(end - start) // TILE) * TILE for start, end in spans)
    return span, total, width


def slice_start(chip, block, chips):
    span, total, width = slice_plan(block, chips)
    start = chip * span // LANES * LANES
    over = start + width - total
    return start - over * ((over + total - 1) // total)


def share_rows(rows):
    return SUBLANES * round(0.6 * rows / SUBLANES)


def fetch_kernel(names, block, *refs):
    count = len(names)
    chips = lax.axis_size("fsdp") // 2
    me, place = lax.axis_index("fsdp"), lax.axis_index("ctx")
    chip, core = me // 2, me % 2
    odd = place % 2
    span, total, width = slice_plan(block, chips)
    srcs = []
    outs = []
    at_in = at_out = 0
    n_in = sum(1 for name in names if name != "up")
    n_out = count
    for name in names:
        if name != "up":
            srcs.append(refs[at_in])
            at_in += 1
        else:
            srcs.append(refs[at_in - 1])
        outs.append(refs[n_in + at_out])
        at_out += 1
    rest = refs[n_in + n_out :]
    stages = rest[:count]
    zero_ref = rest[count]
    xy_send, xy_recv, z_send, z_recv, c_send, c_recv, local_sem, zero_sem = rest[count + 1 :]
    beside = {"ctx": place, "fsdp": chip * 2 + 1 - core}
    across = {"ctx": place + 1 - 2 * odd, "fsdp": me}
    peers = [flipped(chip, step) for step in range(chips)]

    barrier = pltpu.get_barrier_semaphore()
    greeted = [beside, across] + [{"ctx": place, "fsdp": peer * 2 + core} for peer in peers[1:]]
    for target in greeted:
        pl.semaphore_signal(barrier, inc=1, device_id=target, device_id_type=MESH)
    pl.semaphore_wait(barrier, len(greeted))

    def remote(src, dst, send, recv, target):
        return pltpu.make_async_remote_copy(
            src_ref=src,
            dst_ref=dst,
            send_sem=send,
            recv_sem=recv,
            device_id=target,
            device_id_type=MESH,
        )

    def cols(name, peer):
        if name == "all":
            return None
        start = slice_start(peer, block, chips) + (total if name == "up" else 0)
        return pl.ds(pl.multiple_of(start, LANES), width)

    def source(e, first, size, peer):
        window = cols(names[e], peer)
        rows = pl.ds(pl.multiple_of(first, SUBLANES), size)
        return srcs[e].at[rows, :] if window is None else srcs[e].at[rows, window]

    def target_rows(e, owner, first, size):
        rows = srcs[e].shape[0]
        return outs[e].at[pl.ds(pl.multiple_of(owner * rows + first, SUBLANES), size), :]

    rows_like = [e for e in range(count) if names[e] != "pair"]
    pair_like = [e for e in range(count) if names[e] == "pair"]
    waits = []
    xy, zz, c_one, c_two = {}, {}, {}, {}
    for e in rows_like:
        rows = srcs[e].shape[0]
        take = share_rows(rows)
        sub = odd * (rows - take)
        for step in range(1, chips):
            copy = remote(
                source(e, sub, take, peers[step]),
                target_rows(e, me, sub, take),
                xy_send.at[e, step],
                xy_recv.at[e, step],
                {"ctx": place, "fsdp": peers[step] * 2 + core},
            )
            copy.start()
            xy[e, step] = copy
    own = []
    for e in range(count):
        if e in rows_like:
            rows = srcs[e].shape[0]
            src = source(e, 0, rows, chip)
            dst = target_rows(e, me, 0, rows)
        else:
            rows = block
            off = chip * span - slice_start(chip, block, chips)
            src = srcs[e]
            dst = outs[e].at[pl.ds(pl.multiple_of(off + core * block, SUBLANES), rows), :]
        load = pltpu.make_async_copy(src, stages[e], local_sem.at[e, 0])
        load.start()
        copy = remote(src, dst, c_send.at[e, 0, 0], c_recv.at[e, 0, 0], beside)
        copy.start()
        c_one[e, 0] = copy
        own.append((load, dst))
    pad = width - span
    grain = zero_ref.shape[0]
    zeros = []
    for e in pair_like:
        zero_ref[...] = jnp.zeros_like(zero_ref)
        off = chip * span - slice_start(chip, block, chips)
        for i in range(pad // grain):
            past = (i * grain + grain + total - 1 - off) // total
            start = i * grain + span * past
            copy = pltpu.make_async_copy(
                zero_ref,
                outs[e].at[pl.ds(pl.multiple_of(start, SUBLANES), grain), :],
                zero_sem.at[i],
            )
            copy.start()
            zeros.append(copy)
    stores = []
    for e in range(count):
        load, dst = own[e]
        load.wait()
        store = pltpu.make_async_copy(stages[e], dst, local_sem.at[e, 1])
        store.start()
        stores.append(store)

    def after_plane(e):
        rows = srcs[e].shape[0]
        take = share_rows(rows)
        for step in range(1, chips):
            owner = peers[step] * 2 + core
            xy[e, step].wait_recv()
            part = target_rows(e, owner, odd * take, rows - take)
            copy = remote(part, part, z_send.at[e, step], z_recv.at[e, step], across)
            copy.start()
            zz[e, step] = copy
            part = target_rows(e, owner, odd * (rows - take), take)
            copy = remote(part, part, c_send.at[e, step, 0], c_recv.at[e, step, 0], beside)
            copy.start()
            c_one[e, step] = copy

    def after_column(e):
        rows = srcs[e].shape[0]
        take = share_rows(rows)
        for step in range(1, chips):
            owner = peers[step] * 2 + core
            zz[e, step].wait_recv()
            part = target_rows(e, owner, (1 - odd) * take, rows - take)
            copy = remote(part, part, c_send.at[e, step, 1], c_recv.at[e, step, 1], beside)
            copy.start()
            c_two[e, step] = copy

    for i, e in enumerate(rows_like):
        after_plane(e)
        if i > 0:
            after_column(rows_like[i - 1])
    after_column(rows_like[-1])
    for copies in (c_one, c_two):
        for copy in copies.values():
            copy.wait_recv()
    for copies in (xy, zz, c_one, c_two):
        for copy in copies.values():
            copy.wait_send()
    for copy in stores + zeros:
        copy.wait()


def fetch(mesh_sizes, names, values, block, collective_id):
    n_fsdp = mesh_sizes
    chips = n_fsdp // 2
    span, total, width = slice_plan(block, chips)
    count = len(names)
    outs, stages = [], []
    grain = SUBLANES
    at = 0
    for name in names:
        value = values[at - 1] if name == "up" else values[at]
        at += 0 if name == "up" else 1
        rows, columns = value.shape
        if name == "pair":
            outs.append(low_shape(width, columns))
            stages.append((rows, columns))
        else:
            columns = columns if name == "all" else width
            outs.append(low_shape(rows * n_fsdp, columns))
            stages.append((rows, columns))
    pad = width - span
    grain = pad
    for q in range(chips):
        off = q * span - slice_start(q, block, chips)
        while off % grain:
            grain //= 2
    columns = values[-1].shape[1]
    dma = pltpu.SemaphoreType.DMA
    return pl.pallas_call(
        functools.partial(fetch_kernel, names, block),
        in_specs=[pl.BlockSpec(memory_space=pl.ANY)] * len(values),
        out_specs=[pl.BlockSpec(memory_space=pl.ANY)] * count,
        out_shape=outs,
        scratch_shapes=[pltpu.VMEM(shape, jnp.bfloat16) for shape in stages]
        + [pltpu.VMEM((grain, columns), jnp.bfloat16)]
        + [
            dma((count, chips)),
            dma((count, chips)),
            dma((count, chips)),
            dma((count, chips)),
            dma((count, chips, 2)),
            dma((count, chips, 2)),
            dma((count, 2)),
            dma((pad // grain,)),
        ],
        compiler_params=pltpu.CompilerParams(
            collective_id=collective_id, has_side_effects=True, vmem_limit_bytes=VMEM_LIMIT
        ),
        name="fetch_weights",
    )(*values)


def add_low(a, b):
    return (a.astype(jnp.float32) + b.astype(jnp.float32)).astype(jnp.bfloat16)


def ctx_sum_chain(pieces):
    if lax.axis_size("ctx") != 4:
        return [[lax.psum(v, "ctx") for v in piece] for piece in pieces]
    place = lax.axis_index("ctx")
    inside = (place == 1) | (place == 2)
    rounds = (((0, 1), (3, 2)), ((1, 2), (2, 1)), ((1, 0), (2, 3)))
    stage = [list(pieces), [None] * len(pieces), [None] * len(pieces)]
    done = [None] * len(pieces)
    token = None
    for t in range(len(pieces) + 2):
        live = [(r, t - r) for r in range(3) if 0 <= t - r < len(pieces)]
        if token is not None:
            for r, i in live:
                if r == 0:
                    tied = lax.optimization_barrier(tuple(stage[0][i]) + (token,))
                    stage[0][i] = list(tied[:-1])
        moved = [[lax.ppermute(v, "ctx", rounds[r]) for v in stage[r][i]] for r, i in live]
        counts = [len(m) for m in moved]
        flat = lax.optimization_barrier(tuple(v for m in moved for v in m))
        at = 0
        for (r, i), n in zip(live, counts):
            got = flat[at : at + n]
            at += n
            if r < 2:
                stage[r + 1][i] = [add_low(a, b) for a, b in zip(stage[r][i], got)]
            else:
                done[i] = [jnp.where(inside, a, b) for a, b in zip(stage[2][i], got)]
        token = flat[0].reshape(-1)[:1]
    return done


def split_grads(mine, theirs, grad_down, block):
    chips = chip_count()
    width = mine.shape[2]
    rows = mine.shape[1] // chips
    d = grad_down.shape[1]
    me, core = chip_index(), core_index()
    off = me * 2 * block - slice_start(me, block, chips)
    down_mine = lax.dynamic_slice(grad_down, (off + core * block, 0), (block, d))
    down_theirs = lax.dynamic_slice(grad_down, (off + (1 - core) * block, 0), (block, d))
    down = add_low(down_mine, core_swap(down_theirs))
    held = add_low(mine, core_swap(theirs))
    pieces = []
    for step in range(chips):
        piece = lax.dynamic_slice(held, (0, flipped(me, step) * rows, 0), (2, rows, width))
        pieces.append(chip_swap(piece, step) if step else piece)
    half = block // 2 // SUBLANES * SUBLANES
    return [[down[:half]], [pieces[0]], [down[half:]]] + [[p] for p in pieces[1:]]


def join_grads(done, block):
    chips = chip_count()
    down = jnp.concatenate([done[0][0], done[2][0]], axis=0).astype(jnp.float32)
    pieces = [done[1][0]] + [p[0] for p in done[3:]]
    _, rows, width = pieces[0].shape
    span, total, _ = slice_plan(block, chips)
    held = jnp.zeros((chips, 2, rows, width), jnp.bfloat16)
    for step in range(chips):
        held = lax.dynamic_update_slice(
            held, pieces[step][None], (flipped(chip_index(), step), 0, 0, 0)
        )
    starts = [slice_start(q, block, chips) for q in range(chips)]
    runs = []
    for tile in range(total // LANES):
        low, high = tile * LANES, (tile + 1) * LANES
        owners = tuple(q for q in range(chips) if q * span < high and (q + 1) * span > low)
        if runs and runs[-1][0] == owners:
            runs[-1][2] = high
        else:
            runs.append([owners, low, high])
    columns = []
    for half in range(2):
        for owners, low, high in runs:
            terms = [
                held[q, half, :, low - starts[q] : high - starts[q]].astype(jnp.float32)
                for q in owners
            ]
            columns.append(sum(terms[1:], terms[0]))
    return jnp.concatenate(columns, axis=1), down


def tp_forward(hidden_in, gain_vec, weights):
    normed, norm_back = jax.vjp(rms_norm, hidden_in, gain_vec)
    chunks = gather_chunks(normed.astype(jnp.bfloat16))
    first = ffn_fwd(chunks[:1], *weights)
    rest = ffn_fwd(chunks[1:], *weights)
    saved = [[first[i], rest[i]] for i in range(3)]
    return first[3] + rest[3], (norm_back, chunks, *saved)


def tp_grads(grads, retained, weights, rows_d):
    _, chunks, gates, ups, hids = retained
    return ffn_grads(grads, chunks, gates, ups, hids, weights[2], rows_d)


def padded(block, sides, width):
    for axis, dim in sides:
        count = lax.axis_size(axis)
        forward = [(i, i + 1) for i in range(count - 1)]
        backward = [(target, source) for source, target in forward]
        low = lax.ppermute(
            lax.slice_in_dim(block, block.shape[dim] - width, None, axis=dim), axis, forward
        )
        high = lax.ppermute(lax.slice_in_dim(block, 0, width, axis=dim), axis, backward)
        block = jnp.concatenate([low, block, high], axis=dim)
    return block


def rms_norm(values, gain_vec):
    return (
        values * lax.rsqrt(jnp.mean(values * values, axis=-1, keepdims=True) + EPSILON) * gain_vec
    )


def rotary_tables(places):
    exponent = jnp.arange(HEAD_DIM // 2, dtype=jnp.float32) * 2.0 / HEAD_DIM
    inverse = jnp.power(ROPE_BASE, -exponent)
    angles = places.astype(jnp.float32)[:, None] * inverse[None, :]
    angles = jnp.concatenate([angles, angles], axis=-1)
    return (jnp.cos(angles)[:, None, :], jnp.sin(angles)[:, None, :])


def rotary(field_in, cosine, sine_tab):
    half_dim = field_in.shape[-1] // 2
    turned = jnp.concatenate([-field_in[..., half_dim:], field_in[..., :half_dim]], axis=-1)
    return field_in * cosine + turned * sine_tab


def head_parts(mixed_in, q_gain_vec, k_gain_vec, cosine, sine_tab):
    row_count = mixed_in.shape[0]
    q_width = HEADS * HEAD_DIM
    kv_width = KV_HEADS * HEAD_DIM
    queries = mixed_in[:, :q_width].reshape(row_count, HEADS, HEAD_DIM)
    keys_part = mixed_in[:, q_width : q_width + kv_width].reshape(row_count, KV_HEADS, HEAD_DIM)
    values = mixed_in[:, q_width + kv_width :]
    queries = rotary(rms_norm(queries, q_gain_vec), cosine, sine_tab)
    keys_part = rotary(rms_norm(keys_part, k_gain_vec), cosine, sine_tab)
    return (queries.reshape(row_count, q_width), keys_part.reshape(row_count, kv_width), values)


def conv_apply(first_ext, second_ext, kernel):
    half_rows = first_ext.shape[0] - (KERNEL - 1)
    first_out = jnp.zeros((half_rows, first_ext.shape[1]), jnp.float32)
    second_out = jnp.zeros((half_rows, first_ext.shape[1]), jnp.float32)
    for offset in range(KERNEL):
        first_out = first_out + first_ext[offset : offset + half_rows] * kernel[:, offset]
        second_out = second_out + second_ext[offset : offset + half_rows] * kernel[:, offset]
    return jnp.concatenate([first_out, second_out], axis=0)


def matmul(inputs_low, weight):
    return jnp.dot(inputs_low, weight, preferred_element_type=jnp.float32)


def matmul_back(grads_low, weight):
    return lax.dot_general(
        grads_low, weight, (((1,), (1,)), ((), ())), preferred_element_type=jnp.float32
    )


def weight_grad(inputs_low, grads_low):
    return lax.psum_scatter(
        lax.dot_general(
            inputs_low, grads_low, (((0,), (0,)), ((), ())), preferred_element_type=jnp.float32
        ).astype(jnp.bfloat16),
        "fsdp",
        scatter_dimension=0,
        tiled=True,
    )


def score_block(queries_low, key_all):
    row_count = queries_low.shape[0]
    groups = HEADS // KV_HEADS
    query_heads = queries_low.reshape(row_count, KV_HEADS, groups, HEAD_DIM)
    key_heads = key_all.reshape(key_all.shape[0], KV_HEADS, HEAD_DIM)
    raw_scores = jnp.einsum(
        "tkgd,skd->kgts", query_heads, key_heads, preferred_element_type=jnp.float32
    )
    return raw_scores * HEAD_DIM ** (-0.5)


def conv_forward(hidden_in, gain_vec, w_in, kernel_low, w_out):
    width_d = w_out.shape[0]
    normed, norm_back = jax.vjp(rms_norm, hidden_in, gain_vec)
    normed_low = normed.astype(jnp.bfloat16)
    mixed_out = matmul(normed_low, w_in)
    gate_b = mixed_out[:, :width_d]
    gate_c = mixed_out[:, width_d : 2 * width_d]
    inner_val = mixed_out[:, 2 * width_d :]
    product_low = (gate_b * inner_val).astype(jnp.bfloat16)
    row_count = product_low.shape[0]
    half_rows = row_count // 2
    reach = KERNEL - 1
    first_tail = product_low[half_rows - reach : half_rows]
    rim_rows = jnp.concatenate([product_low[row_count - reach :], first_tail], axis=0)
    beside_all = padded(rim_rows, (("ctx", 0),), reach)
    is_last = lax.axis_index("ctx") == lax.axis_size("ctx") - 1
    before_second = jnp.where(is_last, first_tail, beside_all[beside_all.shape[0] - reach :])
    first_ext = jnp.concatenate([beside_all[:reach], product_low[:half_rows]], axis=0).astype(
        jnp.float32
    )
    second_ext = jnp.concatenate([before_second, product_low[half_rows:]], axis=0).astype(
        jnp.float32
    )
    convolved, conv_back = jax.vjp(
        conv_apply, first_ext, second_ext, kernel_low.astype(jnp.float32)
    )
    gated_low = (gate_c * convolved).astype(jnp.bfloat16)
    return (
        matmul(gated_low, w_out),
        (norm_back, normed_low, mixed_out, convolved, conv_back, gated_low, is_last),
    )


def conv_backward(grad_out, retained, w_in, w_out):
    norm_back, normed_low, mixed_out, convolved, conv_back, gated_low, is_last = retained
    width_d = w_out.shape[0]
    gate_b = mixed_out[:, :width_d]
    gate_c = mixed_out[:, width_d : 2 * width_d]
    inner_val = mixed_out[:, 2 * width_d :]
    grads_low = grad_out.astype(jnp.bfloat16)
    grad_w_out = weight_grad(gated_low, grads_low)
    grad_gated = matmul_back(grads_low, w_out)
    grad_c = grad_gated * convolved
    grad_first, grad_second, grad_kernel = conv_back(grad_gated * gate_c)
    reach = KERNEL - 1
    half_rows = grad_first.shape[0] - reach
    to_next = jnp.where(is_last, 0.0, grad_second[:reach])
    sent_rows = jnp.concatenate([grad_first[:reach], to_next], axis=0)
    beside_all = padded(sent_rows, (("ctx", 0),), reach)
    into_first = beside_all[beside_all.shape[0] - reach :] + jnp.where(
        is_last, grad_second[:reach], 0.0
    )
    own_first = grad_first[reach:].at[half_rows - reach :].add(into_first)
    own_second = grad_second[reach:].at[half_rows - reach :].add(beside_all[:reach])
    grad_product = jnp.concatenate([own_first, own_second], axis=0)
    grad_mixed = jnp.concatenate(
        [grad_product * inner_val, grad_c, grad_product * gate_b], axis=1
    ).astype(jnp.bfloat16)
    grad_w_in = weight_grad(normed_low, grad_mixed)
    grad_in, grad_gain = norm_back(matmul_back(grad_mixed, w_in))
    return (grad_out + grad_in, grad_gain, grad_w_in, grad_kernel, grad_w_out)


def attn_forward(hidden_in, gain_vec, w_qkv, q_gain_vec, k_gain_vec, w_out, doc_ids, places):
    row_count = hidden_in.shape[0]
    cosine, sine_tab = rotary_tables(places)
    normed, norm_back = jax.vjp(rms_norm, hidden_in, gain_vec)
    normed_low = normed.astype(jnp.bfloat16)
    mixed_out = matmul(normed_low, w_qkv)
    parts, head_back = jax.vjp(
        functools.partial(head_parts, cosine=cosine, sine_tab=sine_tab),
        mixed_out,
        q_gain_vec,
        k_gain_vec,
    )
    queries_low = parts[0].astype(jnp.bfloat16)
    keys_low = parts[1].astype(jnp.bfloat16)
    values_low = parts[2].astype(jnp.bfloat16)
    own_tags = jnp.stack([doc_ids, places // SPLIT_BASE, places % SPLIT_BASE], axis=1).astype(
        jnp.bfloat16
    )
    key_all, value_all, tag_all = (
        lax.all_gather(keys_low, "ctx", axis=0, tiled=True),
        lax.all_gather(values_low, "ctx", axis=0, tiled=True),
        lax.all_gather(own_tags, "ctx", axis=0, tiled=True),
    )
    tag_int = tag_all.astype(jnp.int32)
    key_doc = tag_int[:, 0]
    key_pos = tag_int[:, 1] * SPLIT_BASE + tag_int[:, 2]
    allowed = (places[:, None] >= key_pos[None, :]) & (doc_ids[:, None] == key_doc[None, :])
    scores = score_block(queries_low, key_all)
    row_peak = jnp.max(jnp.where(allowed, scores, MASKED), axis=-1, keepdims=True)
    log_total = row_peak + jnp.log(
        jnp.sum(jnp.where(allowed, jnp.exp(scores - row_peak), 0.0), axis=-1, keepdims=True)
    )
    weights = jnp.where(allowed, jnp.exp(scores - log_total), 0.0)
    value_heads = value_all.reshape(value_all.shape[0], KV_HEADS, HEAD_DIM)
    attended = jnp.einsum(
        "kgts,skd->tkgd",
        weights.astype(jnp.bfloat16),
        value_heads,
        preferred_element_type=jnp.float32,
    )
    attended_low = attended.reshape(row_count, HEADS * HEAD_DIM).astype(jnp.bfloat16)
    retained = (
        norm_back,
        normed_low,
        head_back,
        queries_low,
        key_all,
        value_heads,
        allowed,
        log_total,
        attended_low,
    )
    return (matmul(attended_low, w_out), retained)


def attn_backward(grad_out, retained, w_qkv, w_out):
    (
        norm_back,
        normed_low,
        head_back,
        queries_low,
        key_all,
        value_heads,
        allowed,
        log_total,
        attended_low,
    ) = retained
    row_count = grad_out.shape[0]
    groups = HEADS // KV_HEADS
    grads_low = grad_out.astype(jnp.bfloat16)
    grad_w_out = weight_grad(attended_low, grads_low)
    att_grad = (
        matmul_back(grads_low, w_out)
        .astype(jnp.bfloat16)
        .reshape(row_count, KV_HEADS, groups, HEAD_DIM)
    )
    scores = score_block(queries_low, key_all)
    weights = jnp.where(allowed, jnp.exp(scores - log_total), 0.0)
    grad_weights = jnp.einsum(
        "tkgd,skd->kgts", att_grad, value_heads, preferred_element_type=jnp.float32
    )
    centre = jnp.sum(weights * grad_weights, axis=-1, keepdims=True)
    score_grad = (weights * (grad_weights - centre)).astype(jnp.bfloat16)
    score_scale = HEAD_DIM ** (-0.5)
    key_heads = key_all.reshape(key_all.shape[0], KV_HEADS, HEAD_DIM)
    query_heads = queries_low.reshape(row_count, KV_HEADS, groups, HEAD_DIM)
    grad_q = (
        jnp.einsum("kgts,skd->tkgd", score_grad, key_heads, preferred_element_type=jnp.float32)
        * score_scale
    )
    grad_k = (
        jnp.einsum("kgts,tkgd->skd", score_grad, query_heads, preferred_element_type=jnp.float32)
        * score_scale
    )
    grad_v = jnp.einsum(
        "kgts,tkgd->skd", weights.astype(jnp.bfloat16), att_grad, preferred_element_type=jnp.float32
    )
    key_count = key_all.shape[0]
    own_k, own_v = (
        lax.psum_scatter(
            grad_k.reshape(key_count, KV_HEADS * HEAD_DIM).astype(jnp.bfloat16),
            "ctx",
            scatter_dimension=0,
            tiled=True,
        ).astype(jnp.float32),
        lax.psum_scatter(
            grad_v.reshape(key_count, KV_HEADS * HEAD_DIM).astype(jnp.bfloat16),
            "ctx",
            scatter_dimension=0,
            tiled=True,
        ).astype(jnp.float32),
    )
    grad_mixed, grad_qg, grad_kg = head_back(
        (grad_q.reshape(row_count, HEADS * HEAD_DIM), own_k, own_v)
    )
    mixed_low = grad_mixed.astype(jnp.bfloat16)
    grad_qkv = weight_grad(normed_low, mixed_low)
    grad_in, grad_gain = norm_back(matmul_back(mixed_low, w_qkv))
    return (grad_out + grad_in, grad_gain, grad_qkv, grad_qg, grad_kg, grad_w_out)


def per_device(
    tokens,
    segments,
    positions,
    out_grad,
    conv_norm,
    conv_in,
    conv_kernel,
    conv_out,
    ffn_norm_1,
    gate_up_1,
    down_1,
    attn_norm,
    qkv_weight,
    q_gain,
    k_gain,
    attn_out,
    ffn_norm_2,
    gate_up_2,
    down_2,
):
    row_count = tokens.shape[1]
    start_rows = tokens.reshape(row_count, tokens.shape[2]).astype(jnp.float32)
    doc_ids = segments.reshape(row_count)
    places = positions.reshape(row_count)
    d = tokens.shape[2]
    block = down_1.shape[0]
    part = conv_norm.shape[0]
    head = q_gain.shape[0]
    size = lax.axis_size("fsdp")
    gains = jnp.concatenate(
        [conv_norm, ffn_norm_1, attn_norm, ffn_norm_2, q_gain, k_gain, conv_kernel.reshape(-1)]
    )
    gains = gather_small(gains)
    g_conv, g_ffn_1, g_attn, g_ffn_2 = (
        gains[:, i * part : (i + 1) * part].reshape(-1).astype(jnp.float32) for i in range(4)
    )
    at = 4 * part
    g_q = gains[:, at : at + head].reshape(-1).astype(jnp.float32)
    g_k = gains[:, at + head : at + 2 * head].reshape(-1).astype(jnp.float32)
    taps = gains[:, at + 2 * head :].reshape(d, KERNEL)

    w_conv_in, w_conv_out, *w_ffn_1 = fetch(
        size,
        ("all", "all", "gate", "up", "pair"),
        (conv_in, conv_out, gate_up_1, down_1),
        block,
        1,
    )
    qkv_weight, attn_out, w_conv_in = lax.optimization_barrier((qkv_weight, attn_out, w_conv_in))
    w_qkv = lax.all_gather(qkv_weight, "fsdp", axis=0, tiled=True)
    w_ao = lax.all_gather(attn_out, "fsdp", axis=0, tiled=True)

    conv_h, conv_saved = conv_forward(start_rows, g_conv, w_conv_in, taps, w_conv_out)
    first_sum = start_rows + conv_h
    parts_1, ffn_saved_1 = tp_forward(first_sum, g_ffn_1, w_ffn_1)
    second_sum = first_sum + scatter_sum(parts_1)
    attn_h, attn_saved = attn_forward(
        second_sum, g_attn, w_qkv, g_q, g_k, w_ao, doc_ids, places
    )
    third_sum = second_sum + attn_h
    gate_up_2, down_2, attn_h = lax.optimization_barrier((gate_up_2, down_2, attn_h))
    w_ffn_2 = fetch(size, ("gate", "up", "pair"), (gate_up_2, down_2), block, 2)
    parts_2, ffn_saved_2 = tp_forward(third_sum, g_ffn_2, w_ffn_2)

    tops = gather_chunks(out_grad.reshape(row_count, d))
    dg, du, *raw_2 = tp_grads(tops, ffn_saved_2, w_ffn_2, part)
    result = (third_sum + scatter_sum(parts_2)).astype(jnp.bfloat16).reshape(tokens.shape)
    back_2 = scatter_sum(ffn_input_grad(dg, du, *w_ffn_2[:2], chip_count()))
    grad_top = out_grad.reshape(row_count, d).astype(jnp.float32)
    grad_in, grad_fn_2 = ffn_saved_2[0](back_2)
    grad_third = grad_top + grad_in
    grad_second, grad_an, grad_qkv, grad_qg, grad_kg, grad_ao = attn_backward(
        grad_third, attn_saved, w_qkv, w_ao
    )
    seconds = gather_chunks(grad_second.astype(jnp.bfloat16))
    dg, du, *raw_1 = tp_grads(seconds, ffn_saved_1, w_ffn_1, part)
    back_1 = scatter_sum(ffn_input_grad(dg, du, *w_ffn_1[:2], chip_count()))
    grad_in, grad_fn_1 = ffn_saved_1[0](back_1)
    grad_first = grad_second + grad_in
    grad_start, grad_cn, grad_cin, grad_ck, grad_cout = conv_backward(
        grad_first, conv_saved, w_conv_in, w_conv_out
    )
    pieces_2 = split_grads(*raw_2, block)
    pieces_1 = split_grads(*raw_1, block)
    pieces = pieces_2 + [[grad_qkv, grad_ao]] + pieces_1 + [[grad_cin, grad_cout]]
    lanes = [ctx_sum_chain(pieces[lane::2]) for lane in range(2)]
    done = [lanes[i % 2][i // 2] for i in range(len(pieces))]
    n_2 = len(pieces_2)
    grad_gu_2, grad_dn_2 = join_grads(done[:n_2], block)
    grad_qkv, grad_ao = done[n_2]
    grad_gu_1, grad_dn_1 = join_grads(done[n_2 + 1 : -1], block)
    grad_cin, grad_cout = done[-1]
    small = sum_small(
        jnp.concatenate(
            [grad_cn, grad_fn_1, grad_an, grad_fn_2, grad_qg, grad_kg, grad_ck.reshape(-1)]
        )
    )
    mine = lax.axis_index("fsdp")
    own = lambda start, count: lax.dynamic_slice(small, (start + mine * count,), (count,))
    totals = (
        own(0, part),
        grad_cin.astype(jnp.float32),
        own(4 * d + 2 * HEAD_DIM, part * KERNEL).reshape(part, KERNEL),
        grad_cout.astype(jnp.float32),
        own(d, part),
        grad_gu_1,
        grad_dn_1,
        own(2 * d, part),
        grad_qkv.astype(jnp.float32),
        own(4 * d, head),
        own(4 * d + HEAD_DIM, head),
        grad_ao.astype(jnp.float32),
        own(3 * d, part),
        grad_gu_2,
        grad_dn_2,
    )
    tokens_grad = grad_start.reshape(tokens.shape)
    return (
        result,
        tokens_grad,
        totals[0],
        totals[1],
        totals[2],
        totals[3],
        totals[4],
        totals[5],
        totals[6],
        totals[7],
        totals[8],
        totals[9],
        totals[10],
        totals[11],
        totals[12],
        totals[13],
        totals[14],
    )


def solution(mesh):
    return jax.shard_map(
        per_device,
        mesh=mesh,
        in_specs=(
            P("fsdp", "ctx", None),
            P("fsdp", "ctx"),
            P("fsdp", "ctx"),
            P("fsdp", "ctx", None),
            P("fsdp"),
            P("fsdp", None),
            P("fsdp", None),
            P("fsdp", None),
            P("fsdp"),
            P("fsdp", None),
            P("fsdp", None),
            P("fsdp"),
            P("fsdp", None),
            P("fsdp"),
            P("fsdp"),
            P("fsdp", None),
            P("fsdp"),
            P("fsdp", None),
            P("fsdp", None),
        ),
        out_specs=(
            P("fsdp", "ctx", None),
            P("fsdp", "ctx", None),
            P("fsdp"),
            P("fsdp", None),
            P("fsdp", None),
            P("fsdp", None),
            P("fsdp"),
            P("fsdp", None),
            P("fsdp", None),
            P("fsdp"),
            P("fsdp", None),
            P("fsdp"),
            P("fsdp"),
            P("fsdp", None),
            P("fsdp"),
            P("fsdp", None),
            P("fsdp", None),
        ),
        check_vma=False,
    )
```
